256 devices in a mesh: dp: 4 (over y), expert: 64 (over z, x, core).
Axes of the slice: x: 4, y: 4, z: 8, core: 2. Of those that a mesh axis runs over, the one named last changes fastest.
Arguments:
- tokens: bfloat16 [131072, 2048], P(('dp', 'expert')), may hold values from -6 to 6
- expert_ids: int32 [131072, 1], P(('dp', 'expert')), may hold values from 0 to 63; in each aligned block of 512 rows (0 to 511, 512 to 1023, ...) at most 16 rows name the same one
- gate_proj: bfloat16 [64, 2048, 768], P('expert'), may hold values from -0.125 to 0.125
- up_proj: bfloat16 [64, 2048, 768], P('expert'), may hold values from -0.125 to 0.125
- down_proj: bfloat16 [64, 768, 2048], P('expert'), may hold values from -0.21875 to 0.21875
Outputs:
- mixed: bfloat16 [131072, 2048], P(('dp', 'expert'))
- slot_index: int32 [131072], P(('dp', 'expert'))
The draws below stay inside these ranges and needn't reach their ends.
Inputs may be any that keep to these rules, and one draw needn't show every extreme that they name: `expert_ids`: among the rows of one device no expert is named more than 16 times; in some devices' rows one expert is named exactly 16 times.
All inputs are finite; a program needn't handle non-finite values.
Results may differ from the reference program's by a relative error of at most 0.0046.
The reference program's roundings to bfloat16 on the way (of `hidden`) count: a program that leaves them out, or rounds other values in their place, can miss the bound.
Values may be sent and summed in bfloat16 or wider, within the bound.
A program may use at most 64 MiB of HBM per device.

```python
import math
import jax
import jax.numpy as jnp
import numpy as np
from jax import lax

D = 2048
FF = 768
TOK_DEV = 512
EXPERTS = 64
TOKENS = 131072
MOST = 16
CAP = 2048


def block_scale(own_key, dims, pieces, least, high):
    loudness, own = 1.0, jax.random.fold_in(own_key, 6)
    for position, blocks in pieces:
        draws = jnp.exp(jax.random.uniform(jax.random.fold_in(own, position), (blocks,), jnp.float32, least / len(pieces), high / len(pieces)))
        loudness = loudness * jnp.repeat(draws, dims[position] // blocks).reshape([-1 if axis == position else 1 for axis in range(len(dims))])
    return loudness


def routed_block(stream_key, own, number, rows, number_of, top, reach, lean):
    sequence = jax.random.permutation(stream_key, number_of)
    crowded, common = portions_of(number_of, rows * top, reach, lean, True), portions_of(number_of, rows * top, reach, lean, False)
    places = jnp.arange(number_of)

    def named(sizes, turn):
        used = int((sizes > 0).sum())
        fixed = max(1, used // 4)
        shifted = fixed + (places - fixed + turn * (used - fixed)) % max(1, number_of - fixed)
        return jnp.zeros((number_of,), jnp.int32).at[sequence[jnp.where(places < fixed, places, shifted)]].set(jnp.asarray(sizes, jnp.int32))

    sizes = jnp.where(number % 4 == 0, named(crowded, number // 4), named(common, number - number // 4 - 1))
    mixed = jax.random.permutation(jax.random.fold_in(own, 3), number_of)
    donor, taker = mixed[0:number_of // 2 * 2:2], mixed[1:number_of // 2 * 2:2]
    slack = jnp.minimum(sizes[donor] - 1, reach - sizes[taker]) // 2
    slack = jnp.where((donor == sequence[0]) | (taker == sequence[0]) | (sizes[taker] == 0), 0, jnp.maximum(slack, 0))
    shifted = jax.random.randint(jax.random.fold_in(own, 4), (number_of // 2,), 0, 1 << 20) % (slack + 1)
    sizes = sizes.at[donor].add(-shifted).at[taker].add(shifted)
    items = jnp.searchsorted(jnp.cumsum(sizes), jnp.arange(rows * top), side="right").astype(jnp.int32)
    table = items.reshape(top, rows).T
    table = table[jax.random.permutation(jax.random.fold_in(own, 1), rows)]
    turn = jax.random.randint(jax.random.fold_in(own, 2), (rows, 1), 0, top)
    return jnp.take_along_axis(table, (jnp.arange(top)[None, :] + turn) % top, axis=1)


def portions_of(number_of, total, most, slope, full):
    weights = [(1 << 20) // math.isqrt(standing ** slope) + 1 for standing in range(1, number_of + 1)]
    largest = most if full else min(most, max(-(-total // number_of), total * weights[0] // sum(weights)))
    least = 1 if total - largest >= number_of - 1 else 0
    holding, rest = [largest] + [least] * (number_of - 1), total - largest - least * (number_of - 1)
    while rest > 0:
        candidates = [i for i in range(1, number_of) if holding[i] < largest] or [i for i in range(1, number_of) if holding[i] < most]
        pool, left = sum([weights[i] for i in candidates]), rest
        for i in candidates:
            more = min(most - holding[i], max(1, left * weights[i] // pool), rest)
            holding[i] = holding[i] + more
            rest = rest - more
    return np.array(holding)


def scatter_about(key, dims, spread, bound, cuts=(), kind=jnp.bfloat16):
    factor_of = block_scale(key, dims, cuts, -0.22, 0.18) if cuts else 1.0
    result = jax.random.normal(key, dims, jnp.float32) * spread * factor_of
    return jnp.minimum(jnp.maximum(result, -bound), bound).astype(kind)


def setup_inputs(seed: int = 0) -> dict:
    arg_keys = jax.random.split(jax.random.key(seed), 6)
    tokens = scatter_about(arg_keys[0], (TOKENS, D), 1.0, 6.0, ((0, 256),))
    expert_ids_keys = jax.random.split(jax.random.fold_in(arg_keys[1], 1), TOKENS // TOK_DEV)
    expert_ids_turns = jax.random.permutation(jax.random.fold_in(arg_keys[1], 3), TOKENS // TOK_DEV)
    expert_ids = jax.vmap(lambda own, number: routed_block(jax.random.fold_in(arg_keys[1], 2), own, number, TOK_DEV, EXPERTS, 1, MOST, 2))(expert_ids_keys, expert_ids_turns).reshape((TOKENS, 1))
    gate_proj = scatter_about(arg_keys[2], (EXPERTS, D, FF), D ** -0.5, 0.125, ((0, 64),))
    up_proj = scatter_about(arg_keys[3], (EXPERTS, D, FF), D ** -0.5, 0.125, ((0, 64),))
    down_proj = scatter_about(arg_keys[4], (EXPERTS, FF, D), FF ** -0.5, 0.21875, ((0, 64),))
    return {"tokens": tokens, "expert_ids": expert_ids, "gate_proj": gate_proj, "up_proj": up_proj, "down_proj": down_proj}


def expert_ffn(args):
    rows, gate_w, up_w, down_w = args
    gate_val = jnp.dot(rows, gate_w, preferred_element_type=jnp.float32)
    up_val = jnp.dot(rows, up_w, preferred_element_type=jnp.float32)
    hidden = (jax.nn.silu(gate_val) * up_val).astype(jnp.bfloat16)
    return jnp.dot(hidden, down_w, preferred_element_type=jnp.float32).astype(jnp.bfloat16)


def reference(tokens, expert_ids, gate_proj, up_proj, down_proj):
    choices = expert_ids[:, 0].astype(jnp.int32)
    onehot = (choices[:, None] == jnp.arange(EXPERTS, dtype=jnp.int32)[None, :]).astype(jnp.int32)
    before = jnp.cumsum(onehot, axis=0) - onehot
    slot_index = jnp.sum(before * onehot, axis=1).astype(jnp.int32)
    is_kept = slot_index < CAP
    buffer = jnp.zeros((EXPERTS, CAP, D), tokens.dtype)
    buffer = buffer.at[choices, slot_index].set(tokens, mode="drop")
    results = lax.map(expert_ffn, (buffer, gate_proj, up_proj, down_proj))
    picked = results[choices, jnp.minimum(slot_index, CAP - 1)]
    mixed = jnp.where(is_kept[:, None], picked, jnp.zeros_like(picked))
    return mixed, slot_index
```

```python
import functools

import jax
import jax.numpy as jnp
from jax import lax
from jax.experimental import pallas as pl
from jax.experimental.pallas import tpu as pltpu
from jax.sharding import PartitionSpec as P

NZ, NX, NC = 8, 4, 2
PLANE = NX * NC
LANES = 128


def offset_of(group):
    half, odd = (group + 1) // 2, group % 2
    return (odd * half + (1 - odd) * (NZ - half)) % NZ


def place(me, group, inner, sign):
    z, x, c = me // PLANE, (me // NC) % NX, me % NC
    dz, dx, dc = offset_of(group), inner // NC, inner % NC
    z = (z + sign * dz + NZ) % NZ
    x = (x + sign * dx + NX) % NX
    c = (c + dc) % NC
    return (z * NX + x) * NC + c


def exchange_kernel(
    out_hbm, counts_ref, gate_hbm, up_hbm, down_hbm,
    back_hbm, offset_ref,
    arrived, result, gate_v, up_v, down_v, count_all, total_mine, total_all,
    w_sem, send_sem, recv_sem, bsend_sem, brecv_sem, csend_sem, crecv_sem, tsend_sem, trecv_sem,
):
    me, mine = lax.axis_index("expert"), lax.axis_index("dp")
    n, dps = lax.axis_size("expert"), lax.axis_size("dp")
    groups = n // PLANE
    most, width = arrived.shape[1], arrived.shape[2]

    for k, (src, dst) in enumerate(((gate_hbm, gate_v), (up_hbm, up_v), (down_hbm, down_v))):
        pltpu.make_async_copy(src.at[0], dst, w_sem.at[k]).start()
    own = pltpu.make_async_copy(out_hbm.at[me], arrived.at[0], recv_sem.at[0])

    barrier = pltpu.get_barrier_semaphore()

    def greet(j, carry):
        pl.semaphore_signal(barrier, inc=1, device_id={"expert": (me + j) % n})
        return carry

    lax.fori_loop(1, n, greet, 0)
    for k in range(1, dps):
        pl.semaphore_signal(barrier, inc=1, device_id={"dp": (mine + k) % dps})
    pl.semaphore_wait(barrier, n - 1 + dps - 1)

    def counts_copy(j):
        return pltpu.make_async_remote_copy(
            src_ref=counts_ref, dst_ref=count_all.at[me],
            send_sem=csend_sem, recv_sem=crecv_sem,
            device_id={"expert": (me + j) % n},
        )

    def send_counts(j, carry):
        counts_copy(j).start()
        return carry

    def tokens_copy(group, inner):
        peer = place(me, group, inner, 1)
        slot = group * PLANE + inner
        return pltpu.make_async_remote_copy(
            src_ref=out_hbm.at[peer], dst_ref=arrived.at[slot],
            send_sem=send_sem.at[slot], recv_sem=recv_sem.at[slot],
            device_id={"expert": peer},
        )

    def back_copy(group, inner):
        peer = place(me, group, inner, -1)
        slot = group * PLANE + inner
        return pltpu.make_async_remote_copy(
            src_ref=result.at[slot], dst_ref=back_hbm.at[me],
            send_sem=bsend_sem.at[slot], recv_sem=brecv_sem.at[slot],
            device_id={"expert": peer},
        )

    def back_arrival(group, inner):
        peer = place(me, group, inner, 1)
        slot = group * PLANE + inner
        return pltpu.make_async_remote_copy(
            src_ref=result.at[slot], dst_ref=back_hbm.at[peer],
            send_sem=bsend_sem.at[slot], recv_sem=brecv_sem.at[slot],
            device_id={"expert": peer},
        )

    lax.fori_loop(1, n, send_counts, 0)

    def issue(*members):
        def body(inner, carry):
            for g in members:
                tokens_copy(g, inner).start()
            return carry
        lax.fori_loop(1 if 0 in members else 0, PLANE, body, 0)

    own.start()
    issue(0)
    for g in range(1, groups - 1, 2):
        issue(g, g + 1)
    issue(groups - 1)

    count_all[me] = counts_ref[...]

    others = count_all.at[pl.ds(1, n - 1)]
    for sem in (crecv_sem, csend_sem):
        pltpu.make_async_copy(others, others, sem).wait()
    rows = count_all[...]
    earlier = lax.broadcasted_iota(jnp.int32, rows.shape, 0) < me
    inner_part = jnp.sum(jnp.where(earlier, rows, 0), axis=0)
    total_mine[...] = jnp.sum(rows, axis=0)

    def total_copy(k):
        return pltpu.make_async_remote_copy(
            src_ref=total_mine, dst_ref=total_all.at[mine],
            send_sem=tsend_sem.at[k], recv_sem=trecv_sem.at[k],
            device_id={"dp": (mine + k) % dps},
        )

    for k in range(1, dps):
        total_copy(k).start()
    total_all[mine] = total_mine[...]

    for k, (src, dst) in enumerate(((gate_hbm, gate_v), (up_hbm, up_v), (down_hbm, down_v))):
        pltpu.make_async_copy(src.at[0], dst, w_sem.at[k]).wait()

    def ffn(group, carry):
        def arrive(inner, carry):
            slot = group * PLANE + inner
            pltpu.make_async_copy(out_hbm.at[0], arrived.at[slot], recv_sem.at[slot]).wait()
            return carry

        lax.fori_loop(0, PLANE, arrive, 0)
        rows = arrived[pl.ds(group * PLANE, PLANE)].reshape(PLANE * most, width)
        gate_val = jnp.dot(rows, gate_v[...], preferred_element_type=jnp.float32)
        up_val = jnp.dot(rows, up_v[...], preferred_element_type=jnp.float32)
        hidden = (jax.nn.silu(gate_val) * up_val).astype(jnp.bfloat16)
        mixed = jnp.dot(hidden, down_v[...], preferred_element_type=jnp.float32)
        result[pl.ds(group * PLANE, PLANE)] = mixed.astype(jnp.bfloat16).reshape(PLANE, most, width)

        def give_back(inner, carry):
            slot = group * PLANE + inner

            @pl.when(slot > 0)
            def _():
                back_copy(group, inner).start()

            @pl.when(slot == 0)
            def _():
                pltpu.make_async_copy(result.at[0], back_hbm.at[me], brecv_sem.at[0]).start()
            return carry

        lax.fori_loop(0, PLANE, give_back, 0)
        return carry

    lax.fori_loop(0, groups, ffn, 0)

    for k in range(1, dps):
        total_copy(k).wait()
    totals = total_all[...]
    before = lax.broadcasted_iota(jnp.int32, totals.shape, 0) < mine
    offset_ref[...] = inner_part + jnp.sum(jnp.where(before, totals, 0), axis=0)

    pltpu.make_async_copy(result.at[0], back_hbm.at[me], brecv_sem.at[0]).wait()

    def finish(slot, carry):
        group, inner = slot // PLANE, slot % PLANE
        tokens_copy(group, inner).wait_send()
        back_copy(group, inner).wait_send()
        back_arrival(group, inner).wait_recv()
        return carry

    lax.fori_loop(1, n, finish, 0)


def exchange(outgoing, counts, gate_proj, up_proj, down_proj):
    n, most, width = outgoing.shape
    dps = lax.axis_size("dp")
    hidden = gate_proj.shape[2]
    vmem, hbm = pl.BlockSpec(memory_space=pltpu.VMEM), pl.BlockSpec(memory_space=pl.ANY)
    return pl.pallas_call(
        exchange_kernel,
        out_shape=(
            jax.ShapeDtypeStruct(outgoing.shape, jnp.bfloat16),
            jax.ShapeDtypeStruct((1, LANES), jnp.int32),
        ),
        in_specs=[hbm, vmem, hbm, hbm, hbm],
        out_specs=(hbm, vmem),
        scratch_shapes=[
            pltpu.VMEM((n, most, width), jnp.bfloat16),
            pltpu.VMEM((n, most, width), jnp.bfloat16),
            pltpu.VMEM((width, hidden), jnp.bfloat16),
            pltpu.VMEM((width, hidden), jnp.bfloat16),
            pltpu.VMEM((hidden, width), jnp.bfloat16),
            pltpu.VMEM((n, 1, LANES), jnp.int32),
            pltpu.VMEM((1, LANES), jnp.int32),
            pltpu.VMEM((dps, 1, LANES), jnp.int32),
            pltpu.SemaphoreType.DMA((3,)),
            pltpu.SemaphoreType.DMA((n,)),
            pltpu.SemaphoreType.DMA((n,)),
            pltpu.SemaphoreType.DMA((n,)),
            pltpu.SemaphoreType.DMA((n,)),
            pltpu.SemaphoreType.DMA,
            pltpu.SemaphoreType.DMA,
            pltpu.SemaphoreType.DMA((dps,)),
            pltpu.SemaphoreType.DMA((dps,)),
        ],
        compiler_params=pltpu.CompilerParams(
            collective_id=0, has_side_effects=True, vmem_limit_bytes=48 * 1024 * 1024
        ),
        cost_estimate=pl.CostEstimate(
            flops=6 * n * most * width * hidden,
            bytes_accessed=3 * width * hidden * 2 + 4 * n * most * width,
            transcendentals=n * most * hidden,
        ),
    )(outgoing, counts, gate_proj, up_proj, down_proj)


def on_device(tokens, expert_ids, gate_proj, up_proj, down_proj):
    tok_rows, width = tokens.shape
    experts_all = lax.axis_size("expert")
    most = 2 * tok_rows // experts_all
    capacity = tok_rows * lax.axis_size("dp")
    choices = expert_ids[:, 0]
    hot = choices[:, None] == jnp.arange(LANES, dtype=jnp.int32)[None, :]
    onehot = hot.astype(jnp.int32)
    counts = jnp.sum(onehot, axis=0)[None, :]
    earlier = jnp.arange(tok_rows)[:, None] > jnp.arange(tok_rows)[None, :]
    before = jnp.dot(
        earlier.astype(jnp.bfloat16), hot.astype(jnp.bfloat16), preferred_element_type=jnp.float32
    )
    local_rank = jnp.sum(jnp.where(hot, before, 0.0), axis=1).astype(jnp.int32)
    position = choices * most + local_rank
    targets = jnp.arange(experts_all * most, dtype=jnp.int32)
    dispatch = (targets[:, None] == position[None, :]).astype(jnp.bfloat16)
    outgoing = jnp.dot(dispatch, tokens, preferred_element_type=jnp.float32).astype(jnp.bfloat16)
    outgoing = outgoing.reshape(experts_all, most, width)
    returned, offset = exchange(outgoing, counts, gate_proj, up_proj, down_proj)
    flat_back = returned.reshape(experts_all * most, width)
    global_slot = (jnp.sum(onehot * offset, axis=1) + local_rank).astype(jnp.int32)
    is_kept = global_slot < capacity
    combine = ((position[:, None] == targets[None, :]) & is_kept[:, None]).astype(jnp.bfloat16)
    mixed = jnp.dot(combine, flat_back, preferred_element_type=jnp.float32)
    return (mixed.astype(jnp.bfloat16), global_slot)


def solution(mesh):
    in_specs = (
        P(("dp", "expert"), None),
        P(("dp", "expert"), None),
        P("expert", None, None),
        P("expert", None, None),
        P("expert", None, None),
    )
    out_specs = (P(("dp", "expert"), None), P(("dp", "expert")))
    return jax.shard_map(
        on_device, mesh=mesh, in_specs=in_specs, out_specs=out_specs, check_vma=False
    )
```

```python
import functools

import jax
import jax.numpy as jnp
from jax import lax
from jax.experimental import pallas as pl
from jax.experimental.pallas import tpu as pltpu
from jax.sharding import PartitionSpec as P

NX, NC = 4, 2
PLANE = NX * NC
LANES = 128
LEVELS = (80, 96, 112)


def mate_of(p, inner, sign):
    x, c = p // NC, p % NC
    x = (x + sign * (inner // NC) + NX) % NX
    c = (c + inner % NC) % NC
    return x * NC + c


def offset_of(group, planes):
    half, odd = (group + 1) // 2, group % 2
    return (odd * half + (1 - odd) * (planes - half)) % planes


def greet(axis, peers, size):
    barrier = pltpu.get_barrier_semaphore()
    for peer in peers:
        pl.semaphore_signal(barrier, inc=1, device_id={axis: peer})


def survey_kernel(
    tokens, places, row, outgoing, meta, offset, largest,
    near, far, mine_sum, sums, asend, arecv, bsend, brecv, csend, crecv,
):
    me, dp = lax.axis_index("expert"), lax.axis_index("dp")
    n, dps = lax.axis_size("expert"), lax.axis_size("dp")
    planes = n // PLANE
    z, p = me // PLANE, me % PLANE
    barrier = pltpu.get_barrier_semaphore()
    greet("expert", [z * PLANE + mate_of(p, i, 1) for i in range(1, PLANE)], n)
    greet("expert", [(z + k) % planes * PLANE + p for k in range(1, planes)], n)
    greet("dp", [(dp + k) % dps for k in range(1, dps)], dps)
    pl.semaphore_wait(barrier, PLANE - 1 + planes - 1 + dps - 1)

    def near_copy(i):
        return pltpu.make_async_remote_copy(
            src_ref=row, dst_ref=near.at[p], send_sem=asend.at[i], recv_sem=arecv.at[i],
            device_id={"expert": z * PLANE + mate_of(p, i, 1)},
        )

    def far_copy(k):
        return pltpu.make_async_remote_copy(
            src_ref=near, dst_ref=far.at[z], send_sem=bsend.at[k], recv_sem=brecv.at[k],
            device_id={"expert": (z + k) % planes * PLANE + p},
        )

    def sum_copy(k):
        return pltpu.make_async_remote_copy(
            src_ref=mine_sum, dst_ref=sums.at[dp], send_sem=csend.at[k], recv_sem=crecv.at[k],
            device_id={"dp": (dp + k) % dps},
        )

    def pack(k, carry):
        at = places[...]
        targets = lax.broadcasted_iota(jnp.int32, (LANES, at.shape[1]), 0) + k * LANES
        dispatch = (targets == at[0:1]).astype(jnp.float32).astype(jnp.bfloat16)
        outgoing[k] = jnp.dot(
            dispatch, tokens[...], preferred_element_type=jnp.float32
        ).astype(jnp.bfloat16)
        marks = jnp.broadcast_to(at[1:2], (8, at.shape[1])).astype(jnp.float32).astype(jnp.bfloat16)
        named = lax.dot_general(
            marks, dispatch, (((1,), (1,)), ((), ())), preferred_element_type=jnp.float32
        )
        meta[k] = named[0:1].astype(jnp.int32) - 1
        return carry

    for i in range(1, PLANE):
        near_copy(i).start()
    near[p] = row[...]
    lax.fori_loop(0, 3, pack, 0)
    for i in range(1, PLANE):
        near_copy(i).wait()
    for k in range(1, planes):
        far_copy(k).start()
    far[z] = near[...]
    lax.fori_loop(3, 6, pack, 0)
    for k in range(1, planes):
        far_copy(k).wait()
    rows = far[...].reshape(n, 1, LANES)
    earlier = lax.broadcasted_iota(jnp.int32, rows.shape, 0) < me
    inner_part = jnp.sum(jnp.where(earlier, rows, 0), axis=0)
    experts_lane = lax.broadcasted_iota(jnp.int32, (1, LANES), 1) < n
    mine_sum[...] = jnp.where(experts_lane, jnp.sum(rows, axis=0), jnp.max(rows, axis=0))
    for k in range(1, dps):
        sum_copy(k).start()
    sums[dp] = mine_sum[...]
    lax.fori_loop(6, planes, pack, 0)
    for k in range(1, dps):
        sum_copy(k).wait()
    totals = sums[...]
    before = lax.broadcasted_iota(jnp.int32, totals.shape, 0) < dp
    offset[...] = inner_part + jnp.sum(jnp.where(before, totals, 0), axis=0)
    largest[...] = jnp.where(experts_lane, 0, jnp.max(totals, axis=0))


def survey(tokens, places, row):
    n, dps = lax.axis_size("expert"), lax.axis_size("dp")
    planes, width = n // PLANE, tokens.shape[1]
    vmem = pl.BlockSpec(memory_space=pltpu.VMEM)
    return pl.pallas_call(
        survey_kernel,
        out_shape=(
            jax.ShapeDtypeStruct((planes, LANES, width), jnp.bfloat16),
            jax.ShapeDtypeStruct((planes, 1, LANES), jnp.int32),
            jax.ShapeDtypeStruct((1, LANES), jnp.int32),
            jax.ShapeDtypeStruct((1, LANES), jnp.int32),
        ),
        in_specs=[vmem] * 3,
        out_specs=(vmem,) * 4,
        scratch_shapes=[
            pltpu.VMEM((PLANE, 1, LANES), jnp.int32),
            pltpu.VMEM((planes, PLANE, 1, LANES), jnp.int32),
            pltpu.VMEM((1, LANES), jnp.int32),
            pltpu.VMEM((dps, 1, LANES), jnp.int32),
            pltpu.SemaphoreType.DMA((PLANE,)),
            pltpu.SemaphoreType.DMA((PLANE,)),
            pltpu.SemaphoreType.DMA((planes,)),
            pltpu.SemaphoreType.DMA((planes,)),
            pltpu.SemaphoreType.DMA((dps,)),
            pltpu.SemaphoreType.DMA((dps,)),
        ],
        compiler_params=pltpu.CompilerParams(
            collective_id=0, has_side_effects=True, vmem_limit_bytes=24 * 1024 * 1024
        ),
    )(tokens, places, row)


def exchange_kernel(
    cap, outgoing, meta, gate_hbm, up_hbm, down_hbm, back_hbm,
    relay, relay_meta, spread, arrived, result, gathered, packed, gate_v, up_v, down_v,
    w_sem, zsend, zrecv, msend, mrecv, xsend, xrecv, rsend, rrecv, bsend, brecv,
):
    me = lax.axis_index("expert")
    n = lax.axis_size("expert")
    planes, most = n // PLANE, arrived.shape[2]
    width = arrived.shape[3]
    z, p = me // PLANE, me % PLANE
    weights = ((gate_hbm, gate_v), (up_hbm, up_v), (down_hbm, down_v))

    def weight_copy(k):
        src, dst = weights[k]
        return pltpu.make_async_copy(src.at[0], dst, w_sem.at[k])

    for k in range(3):
        weight_copy(k).start()
    barrier = pltpu.get_barrier_semaphore()
    greet("expert", [z * PLANE + mate_of(p, i, 1) for i in range(1, PLANE)], n)
    greet("expert", [(z + k) % planes * PLANE + p for k in range(1, planes)], n)
    pl.semaphore_wait(barrier, PLANE - 1 + planes - 1)

    def plane_at(group, sign):
        return (z + sign * offset_of(group, planes) + planes) % planes

    def meta_copy(group):
        to = plane_at(group, 1)
        return pltpu.make_async_remote_copy(
            src_ref=meta.at[to], dst_ref=relay_meta.at[group],
            send_sem=msend.at[group], recv_sem=mrecv.at[group],
            device_id={"expert": to * PLANE + p},
        )

    def bucket_copy(group):
        to = plane_at(group, 1)
        return pltpu.make_async_remote_copy(
            src_ref=outgoing.at[to, pl.ds(0, cap)], dst_ref=relay.at[group],
            send_sem=zsend.at[group], recv_sem=zrecv.at[group],
            device_id={"expert": to * PLANE + p},
        )

    def spread_copy(group, inner):
        mate = mate_of(p, inner, 1)
        at = group * PLANE + inner
        return pltpu.make_async_remote_copy(
            src_ref=spread.at[group, mate], dst_ref=arrived.at[group, p],
            send_sem=xsend.at[at], recv_sem=xrecv.at[at],
            device_id={"expert": z * PLANE + mate},
        )

    def gather_copy(group, inner):
        mate = mate_of(p, inner, -1)
        at = group * PLANE + inner
        return pltpu.make_async_remote_copy(
            src_ref=result.at[group, mate], dst_ref=gathered.at[group, p],
            send_sem=rsend.at[at], recv_sem=rrecv.at[at],
            device_id={"expert": z * PLANE + mate},
        )

    def back_copy(group):
        return pltpu.make_async_remote_copy(
            src_ref=packed.at[group], dst_ref=back_hbm.at[z],
            send_sem=bsend.at[group], recv_sem=brecv.at[group],
            device_id={"expert": plane_at(group, -1) * PLANE + p},
        )

    own_back = pltpu.make_async_copy(packed.at[0], back_hbm.at[z], brecv.at[0])

    def issue(group, carry):
        meta_copy(group).start()
        bucket_copy(group).start()
        return carry

    lax.fori_loop(1, planes, issue, 0)
    relay_meta[0] = meta[z]
    relay[0] = outgoing[z, 0:cap]
    for k in range(3):
        weight_copy(k).wait()

    def routes(group):
        targets = lax.broadcasted_iota(jnp.int32, (PLANE * most, cap), 0)
        named = relay_meta[group][:, 0:cap]
        return (targets == named).astype(jnp.float32).astype(jnp.bfloat16)

    def scatter(group):
        @pl.when(group > 0)
        def _():
            meta_copy(group).wait_recv()
            bucket_copy(group).wait_recv()

        rows = jnp.dot(routes(group), relay[group], preferred_element_type=jnp.float32)
        spread[group] = rows.astype(jnp.bfloat16).reshape(PLANE, most, width)

        def send(inner, carry):
            spread_copy(group, inner).start()
            return carry

        lax.fori_loop(1, PLANE, send, 0)
        arrived[group, p] = spread[group, p]

    def ffn(group):
        def arrive(inner, carry):
            spread_copy(group, inner).wait_recv()
            return carry

        lax.fori_loop(1, PLANE, arrive, 0)
        rows = arrived[group].reshape(PLANE * most, width)
        gate_val = jnp.dot(rows, gate_v[...], preferred_element_type=jnp.float32)
        up_val = jnp.dot(rows, up_v[...], preferred_element_type=jnp.float32)
        hidden = (jax.nn.silu(gate_val) * up_val).astype(jnp.bfloat16)
        mixed = jnp.dot(hidden, down_v[...], preferred_element_type=jnp.float32)
        result[group] = mixed.astype(jnp.bfloat16).reshape(PLANE, most, width)

        def send(inner, carry):
            gather_copy(group, inner).start()
            return carry

        lax.fori_loop(1, PLANE, send, 0)
        gathered[group, p] = result[group, p]

    def give_back(group):
        def arrive(inner, carry):
            gather_copy(group, inner).wait_recv()
            return carry

        lax.fori_loop(1, PLANE, arrive, 0)
        rows = gathered[group].reshape(PLANE * most, width)
        packed[group] = lax.dot_general(
            routes(group), rows, (((0,), (0,)), ((), ())), preferred_element_type=jnp.float32
        ).astype(jnp.bfloat16)

        @pl.when(group > 0)
        def _():
            back_copy(group).start()

        @pl.when(group == 0)
        def _():
            own_back.start()

    def step(i, carry):
        @pl.when(i < planes)
        def _():
            scatter(i)

        @pl.when((i >= 1) & (i <= planes))
        def _():
            ffn(i - 1)

        @pl.when(i >= 2)
        def _():
            give_back(i - 2)

        return carry

    lax.fori_loop(0, planes + 2, step, 0)

    def finish(group, carry):
        meta_copy(group).wait_send()
        bucket_copy(group).wait_send()
        back_copy(group).wait()
        return carry

    def finish_near(at, carry):
        group, inner = at // (PLANE - 1), at % (PLANE - 1) + 1
        spread_copy(group, inner).wait_send()
        gather_copy(group, inner).wait_send()
        return carry

    own_back.wait()
    lax.fori_loop(0, planes * (PLANE - 1), finish_near, 0)
    lax.fori_loop(1, planes, finish, 0)


def exchange(level, cap, most, outgoing, meta, gate_proj, up_proj, down_proj):
    planes, _, width = outgoing.shape
    hidden = gate_proj.shape[2]
    vmem, hbm = pl.BlockSpec(memory_space=pltpu.VMEM), pl.BlockSpec(memory_space=pl.ANY)
    blocks = (planes, PLANE, most, width)
    near = (planes * PLANE,)
    return pl.pallas_call(
        functools.partial(exchange_kernel, cap),
        out_shape=jax.ShapeDtypeStruct((planes, cap, width), jnp.bfloat16),
        in_specs=[vmem, vmem, hbm, hbm, hbm],
        out_specs=hbm,
        scratch_shapes=[
            pltpu.VMEM((planes, cap, width), jnp.bfloat16),
            pltpu.VMEM((planes, 1, LANES), jnp.int32),
            pltpu.VMEM(blocks, jnp.bfloat16),
            pltpu.VMEM(blocks, jnp.bfloat16),
            pltpu.VMEM(blocks, jnp.bfloat16),
            pltpu.VMEM(blocks, jnp.bfloat16),
            pltpu.VMEM((planes, cap, width), jnp.bfloat16),
            pltpu.VMEM((width, hidden), jnp.bfloat16),
            pltpu.VMEM((width, hidden), jnp.bfloat16),
            pltpu.VMEM((hidden, width), jnp.bfloat16),
            pltpu.SemaphoreType.DMA((3,)),
            pltpu.SemaphoreType.DMA((planes,)),
            pltpu.SemaphoreType.DMA((planes,)),
            pltpu.SemaphoreType.DMA((planes,)),
            pltpu.SemaphoreType.DMA((planes,)),
            pltpu.SemaphoreType.DMA(near),
            pltpu.SemaphoreType.DMA(near),
            pltpu.SemaphoreType.DMA(near),
            pltpu.SemaphoreType.DMA(near),
            pltpu.SemaphoreType.DMA((planes,)),
            pltpu.SemaphoreType.DMA((planes,)),
        ],
        compiler_params=pltpu.CompilerParams(
            collective_id=1 + level, has_side_effects=True, vmem_limit_bytes=56 * 1024 * 1024
        ),
    )(outgoing, meta, gate_proj, up_proj, down_proj)


def on_device(tokens, expert_ids, gate_proj, up_proj, down_proj):
    tok_rows, width = tokens.shape
    experts_all = lax.axis_size("expert")
    planes = experts_all // PLANE
    most = 2 * tok_rows // experts_all
    capacity = tok_rows * lax.axis_size("dp")
    choices = expert_ids[:, 0]
    plane = choices // PLANE
    lanes = jnp.arange(LANES, dtype=jnp.int32)[None, :]
    by_expert = lanes == choices[:, None]
    by_plane = lanes == experts_all + plane[:, None]
    hot = (by_expert | by_plane).astype(jnp.bfloat16)
    row = jnp.sum(hot.astype(jnp.int32), axis=0)[None, :]
    earlier = jnp.arange(tok_rows)[:, None] > jnp.arange(tok_rows)[None, :]
    before = jnp.dot(earlier.astype(jnp.bfloat16), hot, preferred_element_type=jnp.float32)
    local_rank = jnp.sum(jnp.where(by_expert, before, 0.0), axis=1).astype(jnp.int32)
    plane_rank = jnp.sum(jnp.where(by_plane, before, 0.0), axis=1).astype(jnp.int32)
    places = jnp.stack(
        [plane * LANES + plane_rank, choices % PLANE * most + local_rank + 1]
    )
    outgoing, meta, offset, largest = survey(tokens, places, row)
    global_slot = jnp.sum(jnp.where(by_expert, offset, 0), axis=1) + local_rank
    is_kept = global_slot < capacity

    def at_capacity(level, cap):
        def run(outgoing, meta, plane, plane_rank, is_kept, gate_proj, up_proj, down_proj):
            back = exchange(level, cap, most, outgoing, meta, gate_proj, up_proj, down_proj)
            position = plane * cap + plane_rank
            targets = jnp.arange(planes * cap, dtype=jnp.int32)
            combine = (position[:, None] == targets[None, :]) & is_kept[:, None]
            mixed = jnp.dot(
                combine.astype(jnp.bfloat16),
                back.reshape(planes * cap, width),
                preferred_element_type=jnp.float32,
            )
            return mixed.astype(jnp.bfloat16)

        return run

    caps = LEVELS + (PLANE * most,)
    need = jnp.max(largest)
    level = sum((need > cap).astype(jnp.int32) for cap in LEVELS)
    mixed = lax.switch(
        level,
        [at_capacity(k, cap) for k, cap in enumerate(caps)],
        outgoing, meta, plane, plane_rank, is_kept, gate_proj, up_proj, down_proj,
    )
    return (mixed, global_slot)


def solution(mesh):
    in_specs = (
        P(("dp", "expert"), None),
        P(("dp", "expert"), None),
        P("expert", None, None),
        P("expert", None, None),
        P("expert", None, None),
    )
    out_specs = (P(("dp", "expert"), None), P(("dp", "expert")))
    return jax.shard_map(
        on_device, mesh=mesh, in_specs=in_specs, out_specs=out_specs, check_vma=False
    )
```

```python
import functools

import jax
import jax.numpy as jnp
from jax import lax
from jax.experimental import pallas as pl
from jax.experimental.pallas import tpu as pltpu
from jax.sharding import PartitionSpec as P

NX, NC = 4, 2
PLANE = NX * NC
LANES = 128
LEVELS = (64, 72, 80, 96)
LAG = 3


def mate_of(p, inner, sign):
    x, c = p // NC, p % NC
    x = (x + sign * (inner // NC) + NX) % NX
    c = (c + inner % NC) % NC
    return x * NC + c


def offset_of(group, planes):
    back = planes - 1 - group
    half, odd = (back + 1) // 2, back % 2
    return (odd * half + (1 - odd) * (planes - half)) % planes


def greet(axis, peers):
    barrier = pltpu.get_barrier_semaphore()
    for peer in peers:
        pl.semaphore_signal(barrier, inc=1, device_id={axis: peer})


def iota(shape, axis):
    return lax.broadcasted_iota(jnp.int32, shape, axis)


def ones_where(mask):
    return mask.astype(jnp.float32).astype(jnp.bfloat16)


def dot(a, b, dims=((1,), (0,))):
    return lax.dot_general(a, b, (dims, ((), ())), preferred_element_type=jnp.float32)


def to_bf16(x):
    return x.astype(jnp.float32).astype(jnp.bfloat16)


def survey_kernel(
    capacity, most, ids_ref, place_ref, slot_ref, merge_ref, meta_ref, level_ref,
    row, near, far, everyone, asend, arecv, bsend, brecv, csend, crecv,
):
    me, dp = lax.axis_index("expert"), lax.axis_index("dp")
    n, dps = lax.axis_size("expert"), lax.axis_size("dp")
    planes, share = n // PLANE, LANES // dps
    z, p = me // PLANE, me % PLANE
    tok_rows = ids_ref.shape[1]
    greet("expert", [z * PLANE + mate_of(p, i, 1) for i in range(1, PLANE)])
    greet("expert", [(z + k) % planes * PLANE + p for k in range(1, planes)])
    greet("dp", [(dp + k) % dps for k in range(1, dps)])

    def near_copy(i):
        return pltpu.make_async_remote_copy(
            src_ref=row, dst_ref=near.at[p], send_sem=asend.at[i], recv_sem=arecv.at[i],
            device_id={"expert": z * PLANE + mate_of(p, i, 1)},
        )

    def far_copy(k):
        return pltpu.make_async_remote_copy(
            src_ref=near, dst_ref=far.at[z], send_sem=bsend.at[k], recv_sem=brecv.at[k],
            device_id={"expert": (z + k) % planes * PLANE + p},
        )

    def dp_copy(k):
        return pltpu.make_async_remote_copy(
            src_ref=far, dst_ref=everyone.at[dp], send_sem=csend.at[k], recv_sem=crecv.at[k],
            device_id={"dp": (dp + k) % dps},
        )

    ids = ids_ref[...]
    named = iota((LANES, tok_rows), 0) == ids
    hot = ones_where(named)
    counts = dot(jnp.ones((8, tok_rows), jnp.bfloat16), hot, ((1,), (1,)))
    row[...] = counts[0:1].astype(jnp.int32)
    pl.semaphore_wait(pltpu.get_barrier_semaphore(), PLANE - 1 + planes - 1 + dps - 1)

    for i in range(1, PLANE):
        near_copy(i).start()
    near[p] = row[...]
    ahead = ones_where(iota((tok_rows, tok_rows), 0) < iota((tok_rows, tok_rows), 1))
    before = dot(hot, ahead)
    rank = jnp.sum(jnp.where(named, before, 0.0), axis=0, keepdims=True).astype(jnp.int32)
    for i in range(1, PLANE):
        near_copy(i).wait()
    for k in range(1, planes):
        far_copy(k).start()
    far[z] = near[...]
    for k in range(1, planes):
        far_copy(k).wait()
    for k in range(1, dps):
        dp_copy(k).start()
    everyone[dp] = far[...]
    for k in range(1, dps):
        dp_copy(k).wait()

    total = dps * n
    table = everyone[...].reshape(total, LANES)
    lower = ones_where(iota((total, total), 1) < iota((total, total), 0))
    ahead_of = dot(lower, to_bf16(table)).astype(jnp.int32)
    kept = jnp.clip(capacity - ahead_of, 0, table)
    of_dps = sum(kept[s * n : (s + 1) * n] for s in range(dps))
    lane, other = iota((LANES, LANES), 0), iota((LANES, LANES), 1)
    same = (lane // PLANE) == (other // PLANE)
    plane_sums = dot(to_bf16(of_dps), ones_where(same)).astype(jnp.int32)
    need = jnp.max((plane_sums + (dps - 1)) // dps)
    level_ref[0] = sum((need > cap).astype(jnp.int32) for cap in LEVELS)

    at = iota((total, LANES), 0)

    def row_of(values, index):
        return jnp.sum(jnp.where(at == index, values, 0), axis=0, keepdims=True)

    keeps = [row_of(kept, s * n + me) for s in range(dps)]
    eight = iota((8, LANES), 0)
    stacked = to_bf16(sum(jnp.where(eight == s, keeps[s], 0) for s in range(dps)))
    within = dot(stacked, ones_where(same & (lane < other))).astype(jnp.int32)
    whole = dot(stacked, ones_where(same)).astype(jnp.int32)
    bases, starts, base = [], [], jnp.zeros((1, LANES), jnp.int32)
    for s in range(dps):
        bases.append(base)
        starts.append(base + within[s : s + 1])
        base = base + whole[s : s + 1]

    def mine(rows):
        return sum(jnp.where(dp == s, rows[s], 0) for s in range(dps))

    lookup = (
        jnp.where(eight == 0, row_of(ahead_of, dp * n + me), 0)
        + jnp.where(eight == 1, mine(starts), 0)
        + jnp.where(eight == 2, mine(bases), 0)
    ).astype(jnp.float32)
    found = lax.dot_general(
        lookup, named.astype(jnp.float32), (((1,), (0,)), ((), ())),
        precision=lax.Precision.HIGHEST, preferred_element_type=jnp.float32,
    ).astype(jnp.int32)
    slot = found[0:1] + rank
    dealt = found[1:2] + rank
    to, at_row = dealt % dps, dealt // dps
    first = (found[2:3] + (dps - 1) - to) // dps
    place = ids // PLANE * LANES + to * share + at_row - first
    slot_ref[...] = slot
    place_ref[...] = jnp.where(slot < capacity, place, -1)

    row_at, lanes = iota((planes, LANES), 0), iota((planes, LANES), 1)

    def column(values, i):
        return jnp.sum(jnp.where(lanes == row_at * PLANE + i, values, 0), axis=1, keepdims=True)

    merge = jnp.zeros((planes, LANES), jnp.int32)
    meta = jnp.zeros((planes, LANES), jnp.int32)
    used = [jnp.zeros((planes, 1), jnp.int32)] * PLANE
    for s in range(dps):
        begin = (column(bases[s], 0) + (dps - 1) - dp) // dps
        merge = merge + jnp.where(lanes // share == s, begin + lanes % share, 0)
        for i in range(PLANE):
            start, many = column(starts[s], i), column(keeps[s], i)
            begin = (start + (dps - 1) - dp) // dps
            end = (start + many + (dps - 1) - dp) // dps
            inside = (lanes >= begin) & (lanes < end)
            meta = meta + jnp.where(inside, i * most + used[i] + lanes - begin + 1, 0)
            used[i] = used[i] + end - begin
    for k in range(planes):
        merge_ref[k] = merge[k : k + 1]
        meta_ref[k] = meta[k : k + 1] - 1


def survey(capacity, most, ids):
    n, dps = lax.axis_size("expert"), lax.axis_size("dp")
    planes, tok_rows = n // PLANE, ids.shape[1]
    vmem = pl.BlockSpec(memory_space=pltpu.VMEM)
    return pl.pallas_call(
        functools.partial(survey_kernel, capacity, most),
        out_shape=(
            jax.ShapeDtypeStruct((1, tok_rows), jnp.int32),
            jax.ShapeDtypeStruct((1, tok_rows), jnp.int32),
            jax.ShapeDtypeStruct((planes, 1, LANES), jnp.int32),
            jax.ShapeDtypeStruct((planes, 1, LANES), jnp.int32),
            jax.ShapeDtypeStruct((1,), jnp.int32),
        ),
        in_specs=[vmem],
        out_specs=(vmem,) * 4 + (pl.BlockSpec(memory_space=pltpu.SMEM),),
        scratch_shapes=[
            pltpu.VMEM((1, LANES), jnp.int32),
            pltpu.VMEM((PLANE, 1, LANES), jnp.int32),
            pltpu.VMEM((planes, PLANE, 1, LANES), jnp.int32),
            pltpu.VMEM((dps, planes, PLANE, 1, LANES), jnp.int32),
            pltpu.SemaphoreType.DMA((PLANE,)),
            pltpu.SemaphoreType.DMA((PLANE,)),
            pltpu.SemaphoreType.DMA((planes,)),
            pltpu.SemaphoreType.DMA((planes,)),
            pltpu.SemaphoreType.DMA((dps,)),
            pltpu.SemaphoreType.DMA((dps,)),
        ],
        compiler_params=pltpu.CompilerParams(
            collective_id=0, has_side_effects=True, vmem_limit_bytes=16 * 1024 * 1024
        ),
    )(ids)


def exchange_kernel(
    cap, tokens, place, merge, meta, gate_hbm, up_hbm, down_hbm, back_hbm,
    dealt, mixed_in, bucket, relay, relay_meta, spread, arrived, result, gathered, packed, home,
    gate_v, up_v, down_v,
    w_sem, ysend, yrecv, zsend, zrecv, msend, mrecv, xsend, xrecv, rsend, rrecv, bsend, brecv,
    hsend, hrecv,
):
    me, dp = lax.axis_index("expert"), lax.axis_index("dp")
    n, dps = lax.axis_size("expert"), lax.axis_size("dp")
    planes, most, width = n // PLANE, arrived.shape[2], arrived.shape[3]
    z, p = me // PLANE, me % PLANE
    last = planes - 1
    weights = ((gate_hbm, gate_v), (up_hbm, up_v), (down_hbm, down_v))

    def weight_copy(k):
        src, dst = weights[k]
        return pltpu.make_async_copy(src.at[0], dst, w_sem.at[k])

    for k in range(3):
        weight_copy(k).start()
    greet("expert", [z * PLANE + mate_of(p, i, 1) for i in range(1, PLANE)])
    greet("expert", [(z + k) % planes * PLANE + p for k in range(1, planes)])
    greet("dp", [(dp + k) % dps for k in range(1, dps)])
    pl.semaphore_wait(pltpu.get_barrier_semaphore(), PLANE - 1 + planes - 1 + dps - 1)

    def plane_at(group, sign):
        return (z + sign * offset_of(group, planes) + planes) % planes

    def deal_copy(group, k):
        to = (dp + k) % dps
        return pltpu.make_async_remote_copy(
            src_ref=dealt.at[group, to], dst_ref=mixed_in.at[group, dp],
            send_sem=ysend.at[group * dps + k], recv_sem=yrecv.at[group * dps + k],
            device_id={"dp": to},
        )

    def home_copy(group, k):
        to = (dp + k) % dps
        return pltpu.make_async_remote_copy(
            src_ref=dealt.at[group, to], dst_ref=back_hbm.at[plane_at(group, 1), dp],
            send_sem=hsend.at[group * dps + k], recv_sem=hrecv.at[group * dps + k],
            device_id={"dp": to},
        )

    def own_home(group):
        return pltpu.make_async_copy(
            dealt.at[group, dp], back_hbm.at[plane_at(group, 1), dp], hrecv.at[group * dps]
        )

    def meta_copy(group):
        to = plane_at(group, 1)
        return pltpu.make_async_remote_copy(
            src_ref=meta.at[to], dst_ref=relay_meta.at[group],
            send_sem=msend.at[group], recv_sem=mrecv.at[group],
            device_id={"expert": to * PLANE + p},
        )

    def bucket_copy(group):
        return pltpu.make_async_remote_copy(
            src_ref=bucket.at[group], dst_ref=relay.at[group],
            send_sem=zsend.at[group], recv_sem=zrecv.at[group],
            device_id={"expert": plane_at(group, 1) * PLANE + p},
        )

    def spread_copy(group, inner):
        mate = mate_of(p, inner, 1)
        at = group * PLANE + inner
        return pltpu.make_async_remote_copy(
            src_ref=spread.at[group, mate], dst_ref=arrived.at[group, p],
            send_sem=xsend.at[at], recv_sem=xrecv.at[at],
            device_id={"expert": z * PLANE + mate},
        )

    def gather_copy(group, inner):
        mate = mate_of(p, inner, -1)
        at = group * PLANE + inner
        return pltpu.make_async_remote_copy(
            src_ref=result.at[group, mate], dst_ref=gathered.at[group, p],
            send_sem=rsend.at[at], recv_sem=rrecv.at[at],
            device_id={"expert": z * PLANE + mate},
        )

    def back_copy(group):
        return pltpu.make_async_remote_copy(
            src_ref=packed.at[group], dst_ref=home.at[group],
            send_sem=bsend.at[group], recv_sem=brecv.at[group],
            device_id={"expert": plane_at(group, -1) * PLANE + p},
        )

    def send_meta(group, carry):
        meta_copy(group).start()
        return carry

    lax.fori_loop(0, last, send_meta, 0)
    relay_meta[last] = meta[z]

    def deal(group, carry):
        at = place[...]
        targets = iota((LANES, at.shape[1]), 0) + plane_at(group, 1) * LANES
        rows = dot(ones_where(targets == at), tokens[...])
        dealt[group] = rows.astype(jnp.bfloat16).reshape(dps, LANES // dps, width)
        for k in range(1, dps):
            deal_copy(group, k).start()
        mixed_in[group, dp] = dealt[group, dp]
        return carry

    lax.fori_loop(0, planes, deal, 0)

    def merging(group):
        return ones_where(iota((cap, LANES), 0) == merge[plane_at(group, 1)])

    def pool(group):
        for k in range(1, dps):
            deal_copy(group, k).wait_recv()
        rows = dot(merging(group), mixed_in[group].reshape(LANES, width)).astype(jnp.bfloat16)

        @pl.when(group < last)
        def _():
            bucket[group] = rows
            bucket_copy(group).start()

        @pl.when(group == last)
        def _():
            relay[last] = rows

    def routes(group):
        named = relay_meta[group][:, 0:cap]
        return ones_where(iota((PLANE * most, cap), 0) == named)

    def scatter(group):
        @pl.when(group < last)
        def _():
            meta_copy(group).wait_recv()
            bucket_copy(group).wait_recv()

        rows = dot(routes(group), relay[group])
        spread[group] = rows.astype(jnp.bfloat16).reshape(PLANE, most, width)

        def send(inner, carry):
            spread_copy(group, inner).start()
            return carry

        lax.fori_loop(1, PLANE, send, 0)
        arrived[group, p] = spread[group, p]

    def ffn(group):
        def arrive(inner, carry):
            spread_copy(group, inner).wait_recv()
            return carry

        lax.fori_loop(1, PLANE, arrive, 0)
        rows = arrived[group].reshape(PLANE * most, width)
        gate_val = dot(rows, gate_v[...])
        up_val = dot(rows, up_v[...])
        hidden = (jax.nn.silu(gate_val) * up_val).astype(jnp.bfloat16)
        mixed = dot(hidden, down_v[...])
        result[group] = mixed.astype(jnp.bfloat16).reshape(PLANE, most, width)

        def send(inner, carry):
            gather_copy(group, inner).start()
            return carry

        lax.fori_loop(1, PLANE, send, 0)
        gathered[group, p] = result[group, p]

    def give_back(group):
        def arrive(inner, carry):
            gather_copy(group, inner).wait_recv()
            return carry

        lax.fori_loop(1, PLANE, arrive, 0)
        rows = gathered[group].reshape(PLANE * most, width)
        rows = dot(routes(group), rows, ((0,), (0,))).astype(jnp.bfloat16)

        @pl.when(group < last)
        def _():
            packed[group] = rows
            back_copy(group).start()

        @pl.when(group == last)
        def _():
            home[last] = rows

    def step(i, carry):
        @pl.when(i < planes)
        def _():
            pool(i)

        @pl.when(i == LAG)
        def _():
            for k in range(3):
                weight_copy(k).wait()

        @pl.when((i >= LAG) & (i < planes + LAG))
        def _():
            scatter(i - LAG)

        @pl.when((i >= LAG + 1) & (i < planes + LAG + 1))
        def _():
            ffn(i - LAG - 1)

        @pl.when(i >= LAG + 2)
        def _():
            give_back(i - LAG - 2)

        return carry

    lax.fori_loop(0, planes + LAG + 2, step, 0)

    def sent_deals(group, carry):
        for k in range(1, dps):
            deal_copy(group, k).wait_send()
        return carry

    lax.fori_loop(0, planes, sent_deals, 0)

    def go_home(i, carry):
        group = (i + last) % planes

        @pl.when(group < last)
        def _():
            back_copy(group).wait_recv()

        rows = dot(merging(group), home[group], ((0,), (0,)))
        dealt[group] = rows.astype(jnp.bfloat16).reshape(dps, LANES // dps, width)
        for k in range(1, dps):
            home_copy(group, k).start()
        own_home(group).start()
        return carry

    lax.fori_loop(0, planes, go_home, 0)

    def finish_near(at, carry):
        group, inner = at // (PLANE - 1), at % (PLANE - 1) + 1
        spread_copy(group, inner).wait_send()
        gather_copy(group, inner).wait_send()
        return carry

    def finish_far(group, carry):
        meta_copy(group).wait_send()
        bucket_copy(group).wait_send()
        back_copy(group).wait_send()
        return carry

    def finish_home(group, carry):
        own_home(group).wait()
        for k in range(1, dps):
            home_copy(group, k).wait()
        return carry

    lax.fori_loop(0, planes * (PLANE - 1), finish_near, 0)
    lax.fori_loop(0, last, finish_far, 0)
    lax.fori_loop(0, planes, finish_home, 0)


def exchange(level, cap, most, tokens, place, merge, meta, gate_proj, up_proj, down_proj):
    planes, width = merge.shape[0], tokens.shape[1]
    dps, hidden = lax.axis_size("dp"), gate_proj.shape[2]
    vmem, hbm = pl.BlockSpec(memory_space=pltpu.VMEM), pl.BlockSpec(memory_space=pl.ANY)
    blocks = pltpu.VMEM((planes, PLANE, most, width), jnp.bfloat16)
    shares = (planes, dps, LANES // dps, width)
    bucket = pltpu.VMEM((planes, cap, width), jnp.bfloat16)
    of_planes = pltpu.SemaphoreType.DMA((planes,))
    of_dps = pltpu.SemaphoreType.DMA((planes * dps,))
    of_plane = pltpu.SemaphoreType.DMA((planes * PLANE,))
    return pl.pallas_call(
        functools.partial(exchange_kernel, cap),
        out_shape=jax.ShapeDtypeStruct(shares, jnp.bfloat16),
        in_specs=[vmem] * 4 + [hbm] * 3,
        out_specs=hbm,
        scratch_shapes=[
            pltpu.VMEM(shares, jnp.bfloat16),
            pltpu.VMEM(shares, jnp.bfloat16),
            bucket,
            bucket,
            pltpu.VMEM((planes, 1, LANES), jnp.int32),
            blocks,
            blocks,
            blocks,
            blocks,
            bucket,
            bucket,
            pltpu.VMEM((width, hidden), jnp.bfloat16),
            pltpu.VMEM((width, hidden), jnp.bfloat16),
            pltpu.VMEM((hidden, width), jnp.bfloat16),
            pltpu.SemaphoreType.DMA((3,)),
            of_dps, of_dps,
            of_planes, of_planes, of_planes, of_planes,
            of_plane, of_plane, of_plane, of_plane,
            of_planes, of_planes,
            of_dps, of_dps,
        ],
        compiler_params=pltpu.CompilerParams(
            collective_id=1 + level, has_side_effects=True, vmem_limit_bytes=58 * 1024 * 1024
        ),
    )(tokens, place, merge, meta, gate_proj, up_proj, down_proj)


def on_device(tokens, expert_ids, gate_proj, up_proj, down_proj):
    tok_rows, width = tokens.shape
    most = 2 * tok_rows // lax.axis_size("expert")
    capacity = tok_rows * lax.axis_size("dp")
    place, slot, merge, meta, level = survey(capacity, most, expert_ids.reshape(1, tok_rows))

    def at_capacity(level, cap):
        return lambda *operands: exchange(level, cap, most, *operands)

    caps = LEVELS + (PLANE * most,)
    back = lax.switch(
        level[0],
        [at_capacity(k, cap) for k, cap in enumerate(caps)],
        tokens, place, merge, meta, gate_proj, up_proj, down_proj,
    ).reshape(-1, width)
    targets = jnp.arange(back.shape[0], dtype=jnp.int32)
    dispatch = (targets[:, None] == place).astype(jnp.bfloat16)
    mixed = lax.dot_general(
        dispatch, back, (((0,), (0,)), ((), ())), preferred_element_type=jnp.float32
    )
    return (mixed.astype(jnp.bfloat16), slot.reshape(tok_rows))


def solution(mesh):
    in_specs = (
        P(("dp", "expert"), None),
        P(("dp", "expert"), None),
        P("expert", None, None),
        P("expert", None, None),
        P("expert", None, None),
    )
    out_specs = (P(("dp", "expert"), None), P(("dp", "expert")))
    return jax.shard_map(
        on_device, mesh=mesh, in_specs=in_specs, out_specs=out_specs, check_vma=False
    )
```

```python
import functools

import jax
import jax.numpy as jnp
from jax import lax
from jax.experimental import pallas as pl
from jax.experimental.pallas import tpu as pltpu
from jax.sharding import PartitionSpec as P

NX, NC = 4, 2
PLANE = NX * NC
LANES = 128
LEVELS = ((72, 24), (80, 24), (80, 32), (128, 32))
ORDER, HANDLED, OWN = (2, 0, 6, 4, 3, 5, 1, 7), (1, 1, 0, 2, 3, 4, 5, 6, 7), 1
HOLE, AHEAD, HOME_LAG = 1, 3, 7


def mate_of(p, inner, sign):
    x, c = p // NC, p % NC
    x = (x + sign * (inner // NC) + NX) % NX
    c = (c + inner % NC) % NC
    return x * NC + c


def entry(table, i):
    n = len(table)
    return table[0] + sum((table[k] - table[k - 1]) * ((i + n - k) // n) for k in range(1, n))


def greet(axis, peers):
    barrier = pltpu.get_barrier_semaphore()
    for peer in peers:
        pl.semaphore_signal(barrier, inc=1, device_id={axis: peer})


def iota(shape, axis):
    return lax.broadcasted_iota(jnp.int32, shape, axis)


def ones_where(mask):
    return mask.astype(jnp.float32).astype(jnp.bfloat16)


def dot(a, b, dims=((1,), (0,))):
    return lax.dot_general(a, b, (dims, ((), ())), preferred_element_type=jnp.float32)


def to_bf16(x):
    return x.astype(jnp.float32).astype(jnp.bfloat16)


def survey_kernel(
    capacity, most, ids_ref, place_ref, slot_ref, merge_ref, meta_ref, level_ref,
    row, near, far, everyone, asend, arecv, bsend, brecv, csend, crecv,
):
    me, dp = lax.axis_index("expert"), lax.axis_index("dp")
    n, dps = lax.axis_size("expert"), lax.axis_size("dp")
    planes, share = n // PLANE, LANES // dps
    z, p = me // PLANE, me % PLANE
    tok_rows = ids_ref.shape[1]
    greet("expert", [z * PLANE + mate_of(p, i, 1) for i in range(1, PLANE)])
    greet("expert", [(z + k) % planes * PLANE + p for k in range(1, planes)])
    greet("dp", [(dp + k) % dps for k in range(1, dps)])

    def near_copy(i):
        return pltpu.make_async_remote_copy(
            src_ref=row, dst_ref=near.at[p], send_sem=asend.at[i], recv_sem=arecv.at[i],
            device_id={"expert": z * PLANE + mate_of(p, i, 1)},
        )

    def far_copy(k):
        return pltpu.make_async_remote_copy(
            src_ref=near, dst_ref=far.at[z], send_sem=bsend.at[k], recv_sem=brecv.at[k],
            device_id={"expert": (z + k) % planes * PLANE + p},
        )

    def dp_copy(k):
        return pltpu.make_async_remote_copy(
            src_ref=far, dst_ref=everyone.at[dp], send_sem=csend.at[k], recv_sem=crecv.at[k],
            device_id={"dp": (dp + k) % dps},
        )

    ids = ids_ref[...]
    named = iota((LANES, tok_rows), 0) == ids
    hot = ones_where(named)
    counts = dot(jnp.ones((8, tok_rows), jnp.bfloat16), hot, ((1,), (1,)))
    row[...] = counts[0:1].astype(jnp.int32)
    pl.semaphore_wait(pltpu.get_barrier_semaphore(), PLANE - 1 + planes - 1 + dps - 1)

    for i in range(1, PLANE):
        near_copy(i).start()
    near[p] = row[...]
    ahead = ones_where(iota((tok_rows, tok_rows), 0) < iota((tok_rows, tok_rows), 1))
    before = dot(hot, ahead)
    rank = jnp.sum(jnp.where(named, before, 0.0), axis=0, keepdims=True).astype(jnp.int32)
    for i in range(1, PLANE):
        near_copy(i).wait()
    for k in range(1, planes):
        far_copy(k).start()
    far[z] = near[...]
    for k in range(1, planes):
        far_copy(k).wait()
    for k in range(1, dps):
        dp_copy(k).start()
    everyone[dp] = far[...]
    for k in range(1, dps):
        dp_copy(k).wait()

    total = dps * n
    table = everyone[...].reshape(total, LANES)
    lower = ones_where(iota((total, total), 1) < iota((total, total), 0))
    ahead_of = dot(lower, to_bf16(table)).astype(jnp.int32)
    kept = jnp.clip(capacity - ahead_of, 0, table)
    lane, other = iota((LANES, LANES), 0), iota((LANES, LANES), 1)
    same = (lane // PLANE) == (other // PLANE)
    plane_sums = dot(to_bf16(kept), ones_where(same)).astype(jnp.int32)

    def largest(values):
        return jnp.max((values + (dps - 1)) // dps)

    def of_dps(values):
        return sum(values[s * n : (s + 1) * n] for s in range(dps))

    needs = (
        largest(of_dps(plane_sums)),
        largest(plane_sums),
    )
    level_ref[0] = sum(
        functools.reduce(jnp.logical_or, [need > cap for need, cap in zip(needs, caps)]).astype(jnp.int32)
        for caps in LEVELS[:-1]
    )

    at = iota((total, LANES), 0)

    def row_of(values, index):
        return jnp.sum(jnp.where(at == index, values, 0), axis=0, keepdims=True)

    keeps = [row_of(kept, s * n + me) for s in range(dps)]
    eight = iota((8, LANES), 0)
    stacked = to_bf16(sum(jnp.where(eight == s, keeps[s], 0) for s in range(dps)))
    within = dot(stacked, ones_where(same & (lane < other))).astype(jnp.int32)
    whole = dot(stacked, ones_where(same)).astype(jnp.int32)
    bases, starts, base = [], [], jnp.zeros((1, LANES), jnp.int32)
    for s in range(dps):
        bases.append(base)
        starts.append(base + within[s : s + 1])
        base = base + whole[s : s + 1]

    def mine(rows):
        return sum(jnp.where(dp == s, rows[s], 0) for s in range(dps))

    lookup = (
        jnp.where(eight == 0, row_of(ahead_of, dp * n + me), 0)
        + jnp.where(eight == 1, mine(starts), 0)
        + jnp.where(eight == 2, mine(bases), 0)
    ).astype(jnp.float32)
    found = lax.dot_general(
        lookup, named.astype(jnp.float32), (((1,), (0,)), ((), ())),
        precision=lax.Precision.HIGHEST, preferred_element_type=jnp.float32,
    ).astype(jnp.int32)
    slot = found[0:1] + rank
    dealt = found[1:2] + rank
    to, at_row = dealt % dps, dealt // dps
    first = (found[2:3] + (dps - 1) - to) // dps
    place = ids // PLANE * LANES + to * share + at_row - first
    slot_ref[...] = slot
    place_ref[...] = jnp.where(slot < capacity, place, -1)

    row_at, lanes = iota((planes, LANES), 0), iota((planes, LANES), 1)

    def column(values, i):
        return jnp.sum(jnp.where(lanes == row_at * PLANE + i, values, 0), axis=1, keepdims=True)

    merge = jnp.zeros((planes, LANES), jnp.int32)
    meta = jnp.zeros((planes, LANES), jnp.int32)
    used = [jnp.zeros((planes, 1), jnp.int32)] * PLANE
    for s in range(dps):
        begin = (column(bases[s], 0) + (dps - 1) - dp) // dps
        merge = merge + jnp.where(lanes // share == s, begin + lanes % share, 0)
        for i in range(PLANE):
            start, many = column(starts[s], i), column(keeps[s], i)
            begin = (start + (dps - 1) - dp) // dps
            end = (start + many + (dps - 1) - dp) // dps
            inside = (lanes >= begin) & (lanes < end)
            meta = meta + jnp.where(inside, i * most + used[i] + lanes - begin + 1, 0)
            used[i] = used[i] + end - begin
    for k in range(planes):
        merge_ref[k] = merge[k : k + 1]
        meta_ref[k] = meta[k : k + 1] - 1


def survey(capacity, most, ids):
    n, dps = lax.axis_size("expert"), lax.axis_size("dp")
    planes, tok_rows = n // PLANE, ids.shape[1]
    vmem = pl.BlockSpec(memory_space=pltpu.VMEM)
    return pl.pallas_call(
        functools.partial(survey_kernel, capacity, most),
        out_shape=(
            jax.ShapeDtypeStruct((1, tok_rows), jnp.int32),
            jax.ShapeDtypeStruct((1, tok_rows), jnp.int32),
            jax.ShapeDtypeStruct((planes, 1, LANES), jnp.int32),
            jax.ShapeDtypeStruct((planes, 1, LANES), jnp.int32),
            jax.ShapeDtypeStruct((1,), jnp.int32),
        ),
        in_specs=[vmem],
        out_specs=(vmem,) * 4 + (pl.BlockSpec(memory_space=pltpu.SMEM),),
        scratch_shapes=[
            pltpu.VMEM((1, LANES), jnp.int32),
            pltpu.VMEM((PLANE, 1, LANES), jnp.int32),
            pltpu.VMEM((planes, PLANE, 1, LANES), jnp.int32),
            pltpu.VMEM((dps, planes, PLANE, 1, LANES), jnp.int32),
            pltpu.SemaphoreType.DMA((PLANE,)),
            pltpu.SemaphoreType.DMA((PLANE,)),
            pltpu.SemaphoreType.DMA((planes,)),
            pltpu.SemaphoreType.DMA((planes,)),
            pltpu.SemaphoreType.DMA((dps,)),
            pltpu.SemaphoreType.DMA((dps,)),
        ],
        compiler_params=pltpu.CompilerParams(
            collective_id=0, has_side_effects=True, vmem_limit_bytes=16 * 1024 * 1024
        ),
    )(ids)


def exchange_kernel(
    caps, tokens, place, merge, meta, gate_hbm, up_hbm, down_hbm, back_hbm,
    dealt, mixed_in, bucket, relay, relay_meta, spread, arrived, result, gathered, packed, home,
    gate_v, up_v, down_v,
    w_sem, ysend, yrecv, zsend, zrecv, msend, mrecv, xsend, xrecv, rsend, rrecv, bsend, brecv,
    hsend, hrecv,
):
    me, dp = lax.axis_index("expert"), lax.axis_index("dp")
    n, dps = lax.axis_size("expert"), lax.axis_size("dp")
    planes, most, width = n // PLANE, arrived.shape[2], arrived.shape[3]
    z, p = me // PLANE, me % PLANE
    cap, share = caps
    some = pl.ds(0, share)
    weights = ((gate_hbm, gate_v), (up_hbm, up_v), (down_hbm, down_v))

    def weight_copy(k):
        src, dst = weights[k]
        return pltpu.make_async_copy(src.at[0], dst, w_sem.at[k])

    for k in range(3):
        weight_copy(k).start()

    def clear(group, carry):
        mixed_in[group] = jnp.zeros(mixed_in.shape[1:], mixed_in.dtype)
        return carry

    lax.fori_loop(0, planes, clear, 0)
    greet("expert", [z * PLANE + mate_of(p, i, 1) for i in range(1, PLANE)])
    greet("expert", [(z + k) % planes * PLANE + p for k in range(1, planes)])
    greet("dp", [(dp + k) % dps for k in range(1, dps)])
    pl.semaphore_wait(pltpu.get_barrier_semaphore(), PLANE - 1 + planes - 1 + dps - 1)

    def plane_at(group, sign):
        return (z + sign * entry(ORDER, group) + planes) % planes

    def deal_copy(group, k):
        to = (dp + k) % dps
        return pltpu.make_async_remote_copy(
            src_ref=dealt.at[group, to, some], dst_ref=mixed_in.at[group, dp, some],
            send_sem=ysend.at[group * dps + k], recv_sem=yrecv.at[group * dps + k],
            device_id={"dp": to},
        )

    def home_copy(group, k):
        to = (dp + k) % dps
        return pltpu.make_async_remote_copy(
            src_ref=dealt.at[group, to, some], dst_ref=back_hbm.at[plane_at(group, 1), dp],
            send_sem=hsend.at[group * dps + k], recv_sem=hrecv.at[group * dps + k],
            device_id={"dp": to},
        )

    def own_home(group):
        return pltpu.make_async_copy(
            dealt.at[group, dp, some], back_hbm.at[plane_at(group, 1), dp], hrecv.at[group * dps]
        )

    def meta_copy(group):
        to = plane_at(group, 1)
        return pltpu.make_async_remote_copy(
            src_ref=meta.at[to], dst_ref=relay_meta.at[group],
            send_sem=msend.at[group], recv_sem=mrecv.at[group],
            device_id={"expert": to * PLANE + p},
        )

    def bucket_copy(group):
        return pltpu.make_async_remote_copy(
            src_ref=bucket.at[group], dst_ref=relay.at[group],
            send_sem=zsend.at[group], recv_sem=zrecv.at[group],
            device_id={"expert": plane_at(group, 1) * PLANE + p},
        )

    def spread_copy(group, inner):
        mate = mate_of(p, inner, 1)
        at = group * PLANE + inner
        return pltpu.make_async_remote_copy(
            src_ref=spread.at[group, mate], dst_ref=arrived.at[group, p],
            send_sem=xsend.at[at], recv_sem=xrecv.at[at],
            device_id={"expert": z * PLANE + mate},
        )

    def gather_copy(group, inner):
        mate = mate_of(p, inner, -1)
        at = group * PLANE + inner
        return pltpu.make_async_remote_copy(
            src_ref=result.at[group, mate], dst_ref=gathered.at[group, p],
            send_sem=rsend.at[at], recv_sem=rrecv.at[at],
            device_id={"expert": z * PLANE + mate},
        )

    def back_copy(group):
        return pltpu.make_async_remote_copy(
            src_ref=packed.at[group], dst_ref=home.at[group],
            send_sem=bsend.at[group], recv_sem=brecv.at[group],
            device_id={"expert": plane_at(group, -1) * PLANE + p},
        )

    def send_meta(group, carry):
        @pl.when(group != OWN)
        def _():
            meta_copy(group).start()

        return carry

    lax.fori_loop(0, planes, send_meta, 0)
    relay_meta[OWN] = meta[z]

    def deal(group, carry):
        at = place[...]
        targets = iota((LANES, at.shape[1]), 0) + plane_at(group, 1) * LANES
        rows = dot(ones_where(targets == at), tokens[...])
        dealt[group] = rows.astype(jnp.bfloat16).reshape(dps, LANES // dps, width)
        for k in range(1, dps):
            deal_copy(group, k).start()
        mixed_in[group, dp] = dealt[group, dp]
        return carry

    lax.fori_loop(0, AHEAD, deal, 0)

    def merging(group):
        return ones_where(iota((cap, LANES), 0) == merge[plane_at(group, 1)])

    def pool(group):
        for k in range(1, dps):
            deal_copy(group, k).wait_recv()
        rows = dot(merging(group), mixed_in[group].reshape(LANES, width)).astype(jnp.bfloat16)

        @pl.when(group != OWN)
        def _():
            bucket[group] = rows
            bucket_copy(group).start()

        @pl.when(group == OWN)
        def _():
            relay[OWN] = rows

    def routes(group):
        named = relay_meta[group][:, 0:cap]
        return ones_where(iota((PLANE * most, cap), 0) == named)

    def scatter(group):
        @pl.when(group != OWN)
        def _():
            meta_copy(group).wait_recv()
            bucket_copy(group).wait_recv()

        rows = dot(routes(group), relay[group])
        spread[group] = rows.astype(jnp.bfloat16).reshape(PLANE, most, width)

        def send(inner, carry):
            spread_copy(group, inner).start()
            return carry

        lax.fori_loop(1, PLANE, send, 0)
        arrived[group, p] = spread[group, p]

    def ffn(group):
        def arrive(inner, carry):
            spread_copy(group, inner).wait_recv()
            return carry

        lax.fori_loop(1, PLANE, arrive, 0)
        rows = arrived[group].reshape(PLANE * most, width)
        gate_val = dot(rows, gate_v[...])
        up_val = dot(rows, up_v[...])
        hidden = (jax.nn.silu(gate_val) * up_val).astype(jnp.bfloat16)
        mixed = dot(hidden, down_v[...])
        result[group] = mixed.astype(jnp.bfloat16).reshape(PLANE, most, width)

        def send(inner, carry):
            gather_copy(group, inner).start()
            return carry

        lax.fori_loop(1, PLANE, send, 0)
        gathered[group, p] = result[group, p]

    def give_back(group):
        def arrive(inner, carry):
            gather_copy(group, inner).wait_recv()
            return carry

        lax.fori_loop(1, PLANE, arrive, 0)
        rows = gathered[group].reshape(PLANE * most, width)
        rows = dot(routes(group), rows, ((0,), (0,))).astype(jnp.bfloat16)

        @pl.when(group != OWN)
        def _():
            packed[group] = rows
            back_copy(group).start()

        @pl.when(group == OWN)
        def _():
            home[OWN] = rows

    def stage(run, at):
        @pl.when((at >= 0) & (at < len(HANDLED)) & (at != HOLE))
        def _():
            run(entry(HANDLED, at))

    def homeward(at):
        @pl.when((at >= 0) & (at < planes))
        def _():
            go_home(entry(HANDLED[:HOLE] + HANDLED[HOLE + 1 :], at))

    def step(i, carry):
        @pl.when(i < planes)
        def _():
            pool(i)

        @pl.when(i + AHEAD < planes)
        def _():
            deal(i + AHEAD, 0)

        @pl.when(i == 1)
        def _():
            for k in range(3):
                weight_copy(k).wait()

        stage(scatter, i - 1)
        stage(ffn, i - 2)
        stage(give_back, i - 3)
        homeward(i - HOME_LAG)
        return carry

    def go_home(group):
        for k in range(1, dps):
            deal_copy(group, k).wait_send()

        @pl.when(group != OWN)
        def _():
            back_copy(group).wait_recv()

        rows = dot(merging(group), home[group], ((0,), (0,)))
        dealt[group] = rows.astype(jnp.bfloat16).reshape(dps, LANES // dps, width)
        for k in range(1, dps):
            home_copy(group, k).start()
        own_home(group).start()

    lax.fori_loop(0, planes + HOME_LAG, step, 0)

    def finish_near(at, carry):
        group, inner = at // (PLANE - 1), at % (PLANE - 1) + 1
        spread_copy(group, inner).wait_send()
        gather_copy(group, inner).wait_send()
        return carry

    def finish_far(group, carry):
        @pl.when(group != OWN)
        def _():
            meta_copy(group).wait_send()
            bucket_copy(group).wait_send()
            back_copy(group).wait_send()

        return carry

    def finish_home(group, carry):
        own_home(group).wait()
        for k in range(1, dps):
            home_copy(group, k).wait()
        return carry

    lax.fori_loop(0, planes * (PLANE - 1), finish_near, 0)
    lax.fori_loop(0, planes, finish_far, 0)
    lax.fori_loop(0, planes, finish_home, 0)


def exchange(level, caps, most, tokens, place, merge, meta, gate_proj, up_proj, down_proj):
    planes, width = merge.shape[0], tokens.shape[1]
    dps, hidden = lax.axis_size("dp"), gate_proj.shape[2]
    vmem, hbm = pl.BlockSpec(memory_space=pltpu.VMEM), pl.BlockSpec(memory_space=pl.ANY)
    blocks = pltpu.VMEM((planes, PLANE, most, width), jnp.bfloat16)
    shares = (planes, dps, LANES // dps, width)
    bucket = pltpu.VMEM((planes, caps[0], width), jnp.bfloat16)
    of_planes = pltpu.SemaphoreType.DMA((planes,))
    of_dps = pltpu.SemaphoreType.DMA((planes * dps,))
    of_plane = pltpu.SemaphoreType.DMA((planes * PLANE,))
    return pl.pallas_call(
        functools.partial(exchange_kernel, caps),
        out_shape=jax.ShapeDtypeStruct((planes, dps, caps[1], width), jnp.bfloat16),
        in_specs=[vmem] * 4 + [hbm] * 3,
        out_specs=hbm,
        scratch_shapes=[
            pltpu.VMEM(shares, jnp.bfloat16),
            pltpu.VMEM(shares, jnp.bfloat16),
            bucket,
            bucket,
            pltpu.VMEM((planes, 1, LANES), jnp.int32),
            blocks,
            blocks,
            blocks,
            blocks,
            bucket,
            bucket,
            pltpu.VMEM((width, hidden), jnp.bfloat16),
            pltpu.VMEM((width, hidden), jnp.bfloat16),
            pltpu.VMEM((hidden, width), jnp.bfloat16),
            pltpu.SemaphoreType.DMA((3,)),
            of_dps, of_dps,
            of_planes, of_planes, of_planes, of_planes,
            of_plane, of_plane, of_plane, of_plane,
            of_planes, of_planes,
            of_dps, of_dps,
        ],
        compiler_params=pltpu.CompilerParams(
            collective_id=1 + level, has_side_effects=True, vmem_limit_bytes=58 * 1024 * 1024
        ),
    )(tokens, place, merge, meta, gate_proj, up_proj, down_proj)


def on_device(tokens, expert_ids, gate_proj, up_proj, down_proj):
    tok_rows, width = tokens.shape
    most = 2 * tok_rows // lax.axis_size("expert")
    capacity = tok_rows * lax.axis_size("dp")
    place, slot, merge, meta, level = survey(capacity, most, expert_ids.reshape(1, tok_rows))

    def at_capacity(level, caps):
        def run(tokens, place, merge, meta, gate_proj, up_proj, down_proj):
            back = exchange(level, caps, most, tokens, place, merge, meta, gate_proj, up_proj, down_proj)
            full = LANES // back.shape[1]
            rows = jnp.where(place < 0, -1, place // full * caps[1] + place % full)
            targets = jnp.arange(back.size // width, dtype=jnp.int32)
            dispatch = lax.optimization_barrier((targets[:, None] == rows).astype(jnp.bfloat16))
            mixed = lax.dot_general(
                dispatch, back.reshape(-1, width), (((0,), (0,)), ((), ())),
                preferred_element_type=jnp.float32,
            )
            return mixed.astype(jnp.bfloat16)

        return run

    mixed = lax.switch(
        level[0],
        [at_capacity(k, caps) for k, caps in enumerate(LEVELS)],
        tokens, place, merge, meta, gate_proj, up_proj, down_proj,
    )
    return (mixed, slot.reshape(tok_rows))


def solution(mesh):
    in_specs = (
        P(("dp", "expert"), None),
        P(("dp", "expert"), None),
        P("expert", None, None),
        P("expert", None, None),
        P("expert", None, None),
    )
    out_specs = (P(("dp", "expert"), None), P(("dp", "expert")))
    return jax.shard_map(
        on_device, mesh=mesh, in_specs=in_specs, out_specs=out_specs, check_vma=False
    )
```
